512 devices in a mesh: roll: 64 (over z, y_lo, core), tensor: 8 (over x, y_hi).
Axes of the slice: x: 4, y: 8 (y_hi: 2, y_lo: 4; y = y_hi * 4 + y_lo), z: 8, core: 2. Of those that a mesh axis runs over, the one named last changes fastest.
Arguments:
- grad_out: bfloat16 [24576, 5120], P('roll', 'tensor'), may hold values from -6 to 6
- out_weight: bfloat16 [5120, 4096], P('roll', 'tensor'), may hold values from -0.078125 to 0.078125
- queries: bfloat16 [24576, 4096], P('roll', 'tensor'), may hold values from -6 to 6
- resp_key: bfloat16 [24576, 1024], P('roll', 'tensor'), may hold values from -5 to 5
- resp_value: bfloat16 [24576, 1024], P('roll', 'tensor'), may hold values from -5 to 5
- prefix_key: bfloat16 [256, 1024], P('roll', 'tensor'), may hold values from -5 to 5
- prefix_value: bfloat16 [256, 1024], P('roll', 'tensor'), may hold values from -5 to 5
- lengths: int32 [64], P('roll'), may hold values from 1 to 384
Outputs:
- grad_query: bfloat16 [24576, 4096], P('roll', 'tensor')
- grad_resp_key: bfloat16 [24576, 1024], P('roll', 'tensor')
- grad_resp_value: bfloat16 [24576, 1024], P('roll', 'tensor')
- grad_prefix_key: float32 [256, 1024], P('roll', 'tensor')
- grad_prefix_value: float32 [256, 1024], P('roll', 'tensor')
The draws below stay inside these ranges and needn't reach their ends.
All inputs are finite; a program needn't handle non-finite values.
Results may differ from the reference program's by a relative error of at most 0.0063.
Values may be sent and summed in bfloat16 or wider, within the bound.
No kernel may reach another device: no remote copies, remote signals or barrier semaphores. Data moves between devices by JAX's collectives and lax.ppermute only.
A program may use at most 64 MiB of HBM per device.

```python
import jax
import jax.numpy as jnp
from jax import lax

D = 5120
HQ = 32
KVH = 8
HD = 128
ROWS = 384
RESPONSES = 64
TOKENS = 24576
PREFIX = 256


def draw_queries(key, part):
    normal_part = jnp.clip(jax.random.normal(jax.random.fold_in(key, 3), (TOKENS, HQ * HD), jnp.float32), -5.0, 5.0)
    return normal_part.astype(jnp.bfloat16)


def draw_prefix_key(key, part):
    normal_part = jnp.clip(jax.random.normal(jax.random.fold_in(key, 5), (PREFIX, KVH * HD), jnp.float32), -5.0, 5.0)
    return normal_part.astype(jnp.bfloat16)


def with_ends(entries, key, low, largest):
    longest = entries.shape.index(max(entries.shape))
    spots = []
    for shift in (0, 1):
        where = [jax.random.randint(jax.random.fold_in(key, axis), (), 0, length) for axis, length in enumerate(entries.shape)]
        where[longest] = (where[longest] + shift) % entries.shape[longest]
        spots.append(tuple(where))
    return entries.at[spots[0]].set(low).at[spots[1]].set(largest)


def block_scale(stream_key, extent, pieces, low, top_value):
    def one(axis_at, shards_of):
        draws = jax.random.uniform(jax.random.fold_in(jax.random.fold_in(stream_key, 6), axis_at), (shards_of,), jnp.float32, low / len(pieces), top_value / len(pieces))
        return jnp.repeat(jnp.exp(draws), extent[axis_at] // shards_of).reshape((-1,) + (1,) * (len(extent) - axis_at - 1))

    loudness = one(*pieces[0])
    for cut in pieces[1:]:
        loudness = loudness * one(*cut)
    return loudness


def noise(rng, shape, spread, reach, shards=(), kind=jnp.bfloat16):
    entries = spread * jax.random.normal(rng, shape, jnp.float32)
    if shards:
        entries = entries * block_scale(rng, shape, shards, -0.22, 0.18)
    return jnp.clip(entries, -reach, reach).astype(kind)


def setup_inputs(seed: int = 0) -> dict:
    streams_of = jax.random.split(jax.random.key(seed), 9)
    return {
        "grad_out": noise(streams_of[0], (TOKENS, D), 1.0, 6.0, ((0, 64), (1, 8))),
        "out_weight": noise(streams_of[1], (D, HQ * HD), D ** -0.5, 0.078125, ((0, 64), (1, 8))),
        "queries": draw_queries(jax.random.fold_in(streams_of[8], 71), 0),
        "resp_key": noise(streams_of[3], (TOKENS, KVH * HD), 1.0, 5.0, ((0, 64), (1, 8))),
        "resp_value": noise(streams_of[4], (TOKENS, KVH * HD), 1.0, 5.0, ((0, 64), (1, 8))),
        "prefix_key": draw_prefix_key(jax.random.fold_in(streams_of[8], 71), 0),
        "prefix_value": noise(streams_of[6], (PREFIX, KVH * HD), 1.0, 5.0, ((0, 64), (1, 8))),
        "lengths": with_ends(jax.random.randint(streams_of[7], (RESPONSES,), 1, ROWS + 1), jax.random.fold_in(streams_of[7], 1), 1, ROWS).astype(jnp.int32),
    }


def response_grads(queries, out_grad, resp_key, resp_value, prefix_key, prefix_value):
    row_count = queries.shape[0]
    prefix_rows = prefix_key.shape[0]
    group_size = HQ // KVH
    score_scale = HD ** -0.5
    highest = lax.Precision.HIGHEST
    all_keys = jnp.concatenate([prefix_key, resp_key], axis=0).astype(jnp.float32)
    all_values = jnp.concatenate([prefix_value, resp_value], axis=0).astype(jnp.float32)
    query_heads = queries.astype(jnp.float32).reshape(row_count, KVH, group_size, HD)
    grad_heads = out_grad.astype(jnp.float32).reshape(row_count, KVH, group_size, HD)
    key_heads = all_keys.reshape(-1, KVH, HD)
    value_heads = all_values.reshape(-1, KVH, HD)
    scores = jnp.einsum("ikgd,jkd->kgij", query_heads, key_heads, precision=highest) * score_scale
    query_place = jnp.arange(row_count, dtype=jnp.int32)[:, None]
    key_place = jnp.arange(key_heads.shape[0], dtype=jnp.int32)[None, :]
    allowed = (key_place < prefix_rows) | (key_place - prefix_rows <= query_place)
    scores = jnp.where(allowed, scores, -jnp.inf)
    row_max = jnp.max(scores, axis=-1, keepdims=True)
    shifted = jnp.exp(scores - row_max)
    soft_weights = shifted / jnp.sum(shifted, axis=-1, keepdims=True)
    weights_low = lax.optimization_barrier(soft_weights.astype(jnp.bfloat16)).astype(jnp.float32)
    prob_grad = jnp.einsum("ikgd,jkd->kgij", grad_heads, value_heads, precision=highest)
    row_delta = jnp.sum(soft_weights * prob_grad, axis=-1, keepdims=True)
    score_grad = soft_weights * (prob_grad - row_delta) * score_scale
    score_low = lax.optimization_barrier(score_grad.astype(jnp.bfloat16)).astype(jnp.float32)
    query_grad = jnp.einsum("kgij,jkd->ikgd", score_low, key_heads, precision=highest)
    key_grad = jnp.einsum("kgij,ikgd->jkd", score_low, query_heads, precision=highest).reshape(-1, KVH * HD)
    value_grad = jnp.einsum("kgij,ikgd->jkd", weights_low, grad_heads, precision=highest).reshape(-1, KVH * HD)
    return (query_grad.reshape(row_count, HQ * HD).astype(jnp.bfloat16),
            key_grad[prefix_rows:].astype(jnp.bfloat16),
            value_grad[prefix_rows:].astype(jnp.bfloat16),
            key_grad[:prefix_rows],
            value_grad[:prefix_rows])


def reference(grad_out, out_weight, queries, resp_key, resp_value, prefix_key, prefix_value, lengths):
    token_count = grad_out.shape[0]
    position = jnp.arange(token_count, dtype=jnp.int32)
    owner_index = position // ROWS
    valid_rows = (position % ROWS < lengths[owner_index]).astype(jnp.float32)
    projected = jnp.dot(grad_out, out_weight, preferred_element_type=jnp.float32)
    out_grad = (projected * valid_rows[:, None]).astype(jnp.bfloat16)

    def one_response(running, response):
        start_row = response * ROWS

        def rows_of(array):
            return lax.dynamic_slice_in_dim(array, start_row, ROWS, 0)

        query_grad, key_grad, value_grad, prefix_key_part, prefix_value_part = response_grads(
            rows_of(queries), rows_of(out_grad), rows_of(resp_key), rows_of(resp_value),
            prefix_key, prefix_value)
        return (running[0] + prefix_key_part, running[1] + prefix_value_part), (query_grad, key_grad, value_grad)

    initial = (jnp.zeros(prefix_key.shape, jnp.float32), jnp.zeros(prefix_value.shape, jnp.float32))
    sums, grads = lax.scan(one_response, initial, jnp.arange(lengths.shape[0], dtype=jnp.int32))
    grad_query = grads[0].reshape(token_count, HQ * HD)
    grad_resp_key = grads[1].reshape(token_count, KVH * HD)
    grad_resp_value = grads[2].reshape(token_count, KVH * HD)
    return grad_query, grad_resp_key, grad_resp_value, sums[0], sums[1]
```

```python
from functools import partial

import jax
import jax.numpy as jnp
from jax import lax
from jax.experimental import pallas as pl
from jax.experimental.pallas import tpu as pltpu
from jax.sharding import Mesh
from jax.sharding import PartitionSpec as P

HD = 128
ROWS = 384
BLOCK = 128
GROUP = 4
PREFIX = 256
SCALE = HD**-0.5
F32 = jnp.float32
BF16 = jnp.bfloat16
ROLL = ("z", "yl", "c")
TENSOR = ("x", "yh")
NZ, NY, NX = 8, 4, 4
NT = (((1,), (1,)), ((), ()))


def swap(v, axis, bit=1):
    size = lax.axis_size(axis)
    return lax.ppermute(v, axis, [(i, i ^ bit) for i in range(size)])


def ring_x(v):
    pairs = []
    for x in range(NX):
        pairs.append((x, (x + 1) % NX))
        pairs.append((NX + x, NX + (x - 1) % NX))
    return lax.ppermute(v, ("c", "x"), pairs)


def ring_z(v):
    pairs = []
    for z in range(NZ):
        pairs.append((2 * z, 2 * ((z + 1) % NZ)))
        pairs.append((2 * z + 1, 2 * ((z - 1) % NZ) + 1))
    return lax.ppermute(v, ("z", "c"), pairs)


def in_pair(mine, other, bit, axis):
    first = jnp.where(bit == 0, mine, other)
    second = jnp.where(bit == 0, other, mine)
    return jnp.concatenate([first, second], axis=axis)


def soft_kernel(q_ref, rk_ref, pkv_ref, *p_refs):
    keys = jnp.concatenate([pkv_ref[:, :HD], rk_ref[...]], axis=0)
    for i, p_ref in enumerate(p_refs):
        low = PREFIX + BLOCK * i
        rows = slice(BLOCK * i, BLOCK * (i + 1))
        queries = jnp.concatenate(
            [q_ref[rows, HD * h : HD * (h + 1)] for h in range(GROUP)], axis=0
        )
        scores = (
            lax.dot_general(keys[: low + BLOCK], queries, NT, preferred_element_type=F32) * SCALE
        )
        open_part = scores[:low]
        key_place = lax.broadcasted_iota(jnp.int32, (BLOCK, GROUP * BLOCK), 0)
        row_place = lax.broadcasted_iota(jnp.int32, (BLOCK, GROUP * BLOCK), 1) % BLOCK
        edge = jnp.where(key_place <= row_place, scores[low:], -jnp.inf)
        top = jnp.maximum(
            jnp.max(open_part, axis=0, keepdims=True), jnp.max(edge, axis=0, keepdims=True)
        )
        open_part = jnp.exp(open_part - top)
        edge = jnp.exp(edge - top)
        total = jnp.sum(open_part, axis=0, keepdims=True) + jnp.sum(edge, axis=0, keepdims=True)
        share = 1.0 / total
        p_ref[:low] = (open_part * share).astype(BF16)
        p_ref[low:] = (edge * share).astype(BF16)


def grad_kernel(
    place_ref,
    length_ref,
    *refs,
):
    g_in, w_in = refs[:8], refs[8:17]
    p_refs = refs[17:20]
    q_ref, rk_ref, rv_ref, pkv_ref = refs[20:24]
    gq_ref, grk_ref, grv_ref, gp_ref = refs[24:28]
    g_buf, w_buf, acc, og, sem = refs[28:]
    x, yh, z, core = place_ref[0], place_ref[1], place_ref[2], place_ref[3]
    way = 1 - 2 * core
    copies = []
    for k, src in enumerate(w_in):
        if k < 7:
            step = (k + 1) // 2
            sign = way if k % 2 == 0 else -way
            slot = lax.rem(z + step * sign + 8, 8)
            dst = w_buf.at[slot]
        else:
            half = core if k == 7 else 1 - core
            slot = lax.rem(z + 4, 8)
            dst = w_buf.at[slot, pl.ds(pl.multiple_of(320 * half, 320), 320)]
        copies.append(pltpu.make_async_copy(src, dst, sem.at[k]))
    for k, src in enumerate(g_in):
        copies.append(pltpu.make_async_copy(src, g_buf.at[k], sem.at[9 + k]))
    for c in copies:
        c.start()
    for c in copies:
        c.wait()

    def project(k, _):
        side = jnp.where(k < 4, yh, 1 - yh)
        source = lax.rem(x - lax.rem(k, 4) * way + 8, 4)
        w = w_buf[2 * source + side]
        part = jnp.dot(g_buf[k], w, preferred_element_type=F32)
        acc[...] = jnp.where(k == 0, part, acc[...] + part)
        return 0

    lax.fori_loop(0, 8, project, 0)
    row = lax.broadcasted_iota(jnp.int32, (ROWS, GROUP * HD), 0)
    og[...] = jnp.where(row < length_ref[0], acc[...], 0.0).astype(BF16)

    keys = jnp.concatenate([pkv_ref[:, :HD], rk_ref[...]], axis=0)
    values = jnp.concatenate([pkv_ref[:, HD:], rv_ref[...]], axis=0)
    keys_t = keys.astype(F32).T.astype(BF16)
    key_grad = [None] * 4
    value_grad = [None] * 4
    for i, p_ref in enumerate(p_refs):
        width = PREFIX + BLOCK * (i + 1)
        rows = slice(BLOCK * i, BLOCK * (i + 1))
        stack = lambda r: jnp.concatenate(
            [r[rows, HD * h : HD * (h + 1)] for h in range(GROUP)], axis=0
        )
        queries, grads = stack(q_ref), stack(og)
        prob_grad = lax.dot_general(values[:width], grads, NT, preferred_element_type=F32)
        weights = p_ref[...]
        wide = weights.astype(F32)
        product = wide * prob_grad
        delta = jnp.sum(product, axis=0, keepdims=True)
        score_low = ((product - wide * delta) * SCALE).astype(BF16)
        kg = jnp.dot(score_low, queries, preferred_element_type=F32)
        vg = jnp.dot(weights, grads, preferred_element_type=F32)
        qt = jnp.dot(keys_t[:, :width], score_low, preferred_element_type=F32)
        for h in range(GROUP):
            gq_ref[rows, HD * h : HD * (h + 1)] = qt[:, BLOCK * h : BLOCK * (h + 1)].T.astype(BF16)
        for j in range(i + 2):
            part = slice(0, PREFIX) if j == 0 else slice(PREFIX + BLOCK * (j - 1), PREFIX + BLOCK * j)
            key_grad[j] = kg[part] if key_grad[j] is None else key_grad[j] + kg[part]
            value_grad[j] = vg[part] if value_grad[j] is None else value_grad[j] + vg[part]
    gp_ref[:, :HD] = key_grad[0]
    gp_ref[:, HD:] = value_grad[0]
    for j in range(3):
        rows = slice(BLOCK * j, BLOCK * (j + 1))
        grk_ref[rows] = key_grad[j + 1].astype(BF16)
        grv_ref[rows] = value_grad[j + 1].astype(BF16)


VM = pl.BlockSpec(memory_space=pltpu.VMEM)
SM = pl.BlockSpec(memory_space=pltpu.SMEM)
ANY = pl.BlockSpec(memory_space=pl.ANY)


def soft(queries, resp_key, prefix):
    return pl.pallas_call(
        soft_kernel,
        out_shape=[
            jax.ShapeDtypeStruct((PREFIX + BLOCK * (i + 1), GROUP * BLOCK), BF16) for i in range(3)
        ],
        in_specs=[VM] * 3,
        out_specs=[VM] * 3,
        cost_estimate=pl.CostEstimate(
            flops=2 * 1536 * 640 * 128, bytes_accessed=3000000, transcendentals=1000000
        ),
        name="soft",
    )(queries, resp_key, prefix)


def grads(place, lengths, g, w, p, queries, resp_key, resp_value, prefix):
    return pl.pallas_call(
        grad_kernel,
        out_shape=[
            jax.ShapeDtypeStruct((ROWS, GROUP * HD), BF16),
            jax.ShapeDtypeStruct((ROWS, HD), BF16),
            jax.ShapeDtypeStruct((ROWS, HD), BF16),
            jax.ShapeDtypeStruct((PREFIX, 2 * HD), F32),
        ],
        in_specs=[SM] * 2 + [ANY] * 17 + [VM] * 7,
        out_specs=[VM] * 4,
        scratch_shapes=[
            pltpu.VMEM((8, ROWS, 640), BF16),
            pltpu.VMEM((8, 640, 512), BF16),
            pltpu.VMEM((ROWS, 512), F32),
            pltpu.VMEM((ROWS, 512), BF16),
            pltpu.SemaphoreType.DMA((17,)),
        ],
        cost_estimate=pl.CostEstimate(
            flops=2 * 384 * 5120 * 512, bytes_accessed=14000000, transcendentals=0
        ),
        name="grads",
    )(place, lengths, *g, *w, *p, queries, resp_key, resp_value, prefix)


def body(grad_out, out_weight, queries, resp_key, resp_value, prefix_key, prefix_value, lengths):
    x, yh = lax.axis_index("x"), lax.axis_index("yh")
    z, yl, core = lax.axis_index("z"), lax.axis_index("yl"), lax.axis_index("c")
    both = jnp.concatenate([prefix_key, prefix_value], axis=1)
    prefix = lax.all_to_all(
        jnp.broadcast_to(both[None], (64,) + both.shape), ROLL, 0, 0, tiled=True
    ).reshape(PREFIX, 2 * HD)

    g = [grad_out]
    for _ in range(3):
        g.append(ring_x(g[-1]))
    other = swap(grad_out, "yh")
    g.append(other)
    for _ in range(3):
        g.append(ring_x(g[-1]))

    two = in_pair(out_weight, swap(out_weight, "yl", 1), yl % 2, 0)
    four = in_pair(two, swap(two, "yl", 2), yl // 2, 0)
    piece = in_pair(
        four.reshape(4, 1, 80, 512), swap(four, "c").reshape(4, 1, 80, 512), core, 1
    ).reshape(640, 512)
    w = [piece]
    ahead = piece
    for _ in range(3):
        ahead = ring_z(ahead)
        w += [ahead, swap(ahead, "c")]
    half = jnp.where(core == 0, ahead[:320], ahead[320:])
    last = ring_z(half)
    w += [last, swap(last, "c")]

    p = soft(queries, resp_key, prefix)
    place = jnp.stack([x, yh, z, core]).astype(jnp.int32)
    gq, grk, grv, gp = grads(
        place, lengths, g, w, p, queries, resp_key, resp_value, prefix
    )
    parts = lax.all_to_all(gp.reshape(64, 4, 2 * HD), ROLL, 0, 0, tiled=True)
    total = jnp.sum(parts, axis=0)
    return gq, grk, grv, total[:, :HD], total[:, HD:]


def solution(mesh):
    torus = Mesh(mesh.devices.reshape(NZ, NY, 2, NX, 2), ROLL + TENSOR)
    placed = P(ROLL, TENSOR)
    return jax.shard_map(
        body,
        mesh=torus,
        in_specs=(placed,) * 7 + (P(ROLL),),
        out_specs=(placed,) * 5,
        check_vma=False,
    )
```

```python
import jax
import jax.numpy as jnp
from jax import lax
from jax.experimental import pallas as pl
from jax.experimental.pallas import tpu as pltpu
from jax.sharding import Mesh
from jax.sharding import PartitionSpec as P

HD = 128
ROWS = 384
BLOCK = 128
GROUP = 4
PREFIX = 256
SCALE = HD**-0.5
F32 = jnp.float32
BF16 = jnp.bfloat16
ROLL = ("z", "yl", "c")
TENSOR = ("x", "yh")
NZ, NY, NX = 8, 4, 4
NT = (((1,), (1,)), ((), ()))


def swap(v, axis, bit=1):
    size = lax.axis_size(axis)
    return lax.ppermute(v, axis, [(i, i ^ bit) for i in range(size)])


def ring_x(v):
    pairs = []
    for x in range(NX):
        pairs.append((x, (x + 1) % NX))
        pairs.append((NX + x, NX + (x - 1) % NX))
    return lax.ppermute(v, ("c", "x"), pairs)


def ring_z(v):
    pairs = []
    for z in range(NZ):
        pairs.append((2 * z, 2 * ((z + 1) % NZ)))
        pairs.append((2 * z + 1, 2 * ((z - 1) % NZ) + 1))
    return lax.ppermute(v, ("z", "c"), pairs)


def in_pair(mine, other, bit, axis):
    first = jnp.where(bit == 0, mine, other)
    second = jnp.where(bit == 0, other, mine)
    return jnp.concatenate([first, second], axis=axis)


def stacked(ref, i):
    rows = slice(BLOCK * i, BLOCK * (i + 1))
    return jnp.concatenate([ref[rows, HD * h : HD * (h + 1)] for h in range(GROUP)], axis=0)


def soft_kernel(q_ref, rk_ref, pkv_ref, *p_refs):
    keys = jnp.concatenate([pkv_ref[:, :HD], rk_ref[...]], axis=0)
    for i, p_ref in enumerate(p_refs):
        low = PREFIX + BLOCK * i
        scores = (
            lax.dot_general(keys[: low + BLOCK], stacked(q_ref, i), NT, preferred_element_type=F32)
            * SCALE
        )
        open_part = scores[:low]
        key_place = lax.broadcasted_iota(jnp.int32, (BLOCK, GROUP * BLOCK), 0)
        row_place = lax.broadcasted_iota(jnp.int32, (BLOCK, GROUP * BLOCK), 1) % BLOCK
        edge = jnp.where(key_place <= row_place, scores[low:], -jnp.inf)
        top = jnp.maximum(
            jnp.max(open_part, axis=0, keepdims=True), jnp.max(edge, axis=0, keepdims=True)
        )
        open_part = jnp.exp(open_part - top)
        edge = jnp.exp(edge - top)
        total = jnp.sum(open_part, axis=0, keepdims=True) + jnp.sum(edge, axis=0, keepdims=True)
        share = 1.0 / total
        p_ref[:low] = open_part * share
        p_ref[low:] = edge * share


def project_kernel(place_ref, *refs):
    g_in, w_in = refs[:7], refs[7:16]
    acc, w_last = refs[16:18]
    g_buf, w_buf, sem = refs[18:]
    x, yh, z, core = place_ref[0], place_ref[1], place_ref[2], place_ref[3]
    way = 1 - 2 * core
    w_copies = []
    for k, src in enumerate(w_in):
        if k < 7:
            step = (k + 1) // 2
            sign = way if k % 2 == 0 else -way
            dst = w_buf.at[lax.rem(z + step * sign + 8, 8)]
        else:
            half = core if k == 7 else 1 - core
            dst = w_buf.at[lax.rem(z + 4, 8), pl.ds(pl.multiple_of(320 * half, 320), 320)]
        w_copies.append(pltpu.make_async_copy(src, dst, sem.at[k]))
    g_copies = [
        pltpu.make_async_copy(src, g_buf.at[k], sem.at[9 + k]) for k, src in enumerate(g_in)
    ]
    for c in w_copies + g_copies:
        c.start()
    for c in w_copies + g_copies:
        c.wait()

    def block_of(k):
        side = jnp.where(k < 4, yh, 1 - yh)
        return 2 * lax.rem(x - lax.rem(k, 4) * way + 8, 4) + side

    acc[...] = jnp.dot(g_buf[0], w_buf[block_of(0)], preferred_element_type=F32)

    def project(k, _):
        acc[...] += jnp.dot(g_buf[k], w_buf[block_of(k)], preferred_element_type=F32)
        return 0

    lax.fori_loop(1, 7, project, 0)
    w_last[...] = w_buf[block_of(7)]


def front_kernel(length_ref, acc, g_last, w_last, p0, p1, p2, q_ref, rv_ref, pkv_ref, gp_ref, og_ref, s0, s1, s2):
    total = acc[...] + jnp.dot(g_last[...], w_last[...], preferred_element_type=F32)
    row = lax.broadcasted_iota(jnp.int32, (ROWS, GROUP * HD), 0)
    out_grad = jnp.where(row < length_ref[0], total, 0.0).astype(BF16)
    for i in range(3):
        for h in range(GROUP):
            at = GROUP * BLOCK * i + BLOCK * h
            og_ref[at : at + BLOCK] = out_grad[
                BLOCK * i : BLOCK * (i + 1), HD * h : HD * (h + 1)
            ]
    values = jnp.concatenate([pkv_ref[:, HD:], rv_ref[...]], axis=0)
    key_grad = jnp.zeros((PREFIX, HD), F32)
    value_grad = jnp.zeros((PREFIX, HD), F32)
    for i, (p_ref, s_ref) in enumerate(zip((p0, p1, p2), (s0, s1, s2))):
        width = PREFIX + BLOCK * (i + 1)
        grads = og_ref[GROUP * BLOCK * i : GROUP * BLOCK * (i + 1)]
        prob_grad = lax.dot_general(values[:width], grads, NT, preferred_element_type=F32)
        weights = p_ref[...]
        delta = jnp.sum(weights * prob_grad, axis=0, keepdims=True)
        score_low = (weights * (prob_grad - delta) * SCALE).astype(BF16)
        s_ref[...] = score_low
        key_grad += jnp.dot(score_low[:PREFIX], stacked(q_ref, i), preferred_element_type=F32)
        value_grad += jnp.dot(weights[:PREFIX].astype(BF16), grads, preferred_element_type=F32)
    for j in range(PREFIX // 4):
        gp_ref[j, :, :HD] = key_grad[4 * j : 4 * j + 4]
        gp_ref[j, :, HD:] = value_grad[4 * j : 4 * j + 4]


def back_kernel(og_ref, s0, s1, s2, p0, p1, p2, q_ref, rk_ref, pkv_ref, gq_ref, grk_ref, grv_ref):
    keys = jnp.concatenate([pkv_ref[:, :HD], rk_ref[...]], axis=0)
    keys_t = keys.astype(F32).T.astype(BF16)
    key_grad = [None] * 3
    value_grad = [None] * 3
    for i, (p_ref, s_ref) in enumerate(zip((p0, p1, p2), (s0, s1, s2))):
        width = PREFIX + BLOCK * (i + 1)
        rows = slice(BLOCK * i, BLOCK * (i + 1))
        score_low = s_ref[...]
        weights = p_ref[PREFIX:].astype(BF16)
        grads = og_ref[GROUP * BLOCK * i : GROUP * BLOCK * (i + 1)]
        kg = jnp.dot(score_low[PREFIX:], stacked(q_ref, i), preferred_element_type=F32)
        vg = jnp.dot(weights, grads, preferred_element_type=F32)
        qt = jnp.dot(keys_t[:, :width], score_low, preferred_element_type=F32)
        for h in range(GROUP):
            gq_ref[rows, HD * h : HD * (h + 1)] = qt[:, BLOCK * h : BLOCK * (h + 1)].T.astype(BF16)
        for j in range(i + 1):
            part = slice(BLOCK * j, BLOCK * (j + 1))
            key_grad[j] = kg[part] if key_grad[j] is None else key_grad[j] + kg[part]
            value_grad[j] = vg[part] if value_grad[j] is None else value_grad[j] + vg[part]
    for j in range(3):
        rows = slice(BLOCK * j, BLOCK * (j + 1))
        grk_ref[rows] = key_grad[j].astype(BF16)
        grv_ref[rows] = value_grad[j].astype(BF16)


VM = pl.BlockSpec(memory_space=pltpu.VMEM)
SM = pl.BlockSpec(memory_space=pltpu.SMEM)
ANY = pl.BlockSpec(memory_space=pl.ANY)
WIDTHS = tuple(PREFIX + BLOCK * (i + 1) for i in range(3))


def call(kernel, outs, in_specs, args, flops, scratch=()):
    return pl.pallas_call(
        kernel,
        out_shape=[jax.ShapeDtypeStruct(s, d) for s, d in outs],
        in_specs=in_specs,
        out_specs=[VM] * len(outs),
        scratch_shapes=scratch,
        cost_estimate=pl.CostEstimate(flops=flops, bytes_accessed=4000000, transcendentals=0),
    )(*args)


def soft(queries, resp_key, prefix):
    outs = [((w, GROUP * BLOCK), F32) for w in WIDTHS]
    return call(soft_kernel, outs, [VM] * 3, (queries, resp_key, prefix), 1 << 30)


def project(place, g, w):
    return call(
        project_kernel,
        [((ROWS, 512), F32), ((640, 512), BF16)],
        [SM] + [ANY] * 16,
        (place, *g, *w),
        2 * 384 * 5120 * 512,
        [
            pltpu.VMEM((7, ROWS, 640), BF16),
            pltpu.VMEM((8, 640, 512), BF16),
            pltpu.SemaphoreType.DMA((16,)),
        ],
    )


def front(lengths, acc, g_last, w_last, p, queries, resp_value, prefix):
    outs = [((64, 4, 2 * HD), F32), ((GROUP * ROWS, HD), BF16)]
    outs += [((w, GROUP * BLOCK), BF16) for w in WIDTHS]
    args = (lengths, acc, g_last, w_last, *p, queries, resp_value, prefix)
    return call(front_kernel, outs, [SM] + [VM] * 9, args, 1 << 30)


def back(og, s, p, queries, resp_key, prefix):
    outs = [((ROWS, GROUP * HD), BF16), ((ROWS, HD), BF16), ((ROWS, HD), BF16)]
    return call(back_kernel, outs, [VM] * 10, (og, *s, *p, queries, resp_key, prefix), 1 << 30)


def steps(grad_out, out_weight, queries, resp_key, resp_value, prefix_key, prefix_value, lengths):
    x, yh = lax.axis_index("x"), lax.axis_index("yh")
    z, yl, core = lax.axis_index("z"), lax.axis_index("yl"), lax.axis_index("c")
    both = jnp.concatenate([prefix_key, prefix_value], axis=1)
    prefix = lax.all_to_all(
        jnp.broadcast_to(both[None], (64,) + both.shape), ROLL, 0, 0, tiled=True
    ).reshape(PREFIX, 2 * HD)

    g = [grad_out]
    for _ in range(3):
        g.append(ring_x(g[-1]))
    g.append(swap(grad_out, "yh"))
    for _ in range(3):
        g.append(ring_x(g[-1]))

    two = in_pair(out_weight, swap(out_weight, "yl", 1), yl % 2, 0)
    four = in_pair(two, swap(two, "yl", 2), yl // 2, 0)
    piece = in_pair(
        four.reshape(4, 1, 80, 512),
        swap(four, "c").reshape(4, 1, 80, 512),
        core,
        1,
    ).reshape(640, 512)
    w = [piece]
    ahead = piece
    for _ in range(3):
        ahead = ring_z(ahead)
        w += [ahead, swap(ahead, "c")]
    half = jnp.where(core == 0, ahead[:320], ahead[320:])
    last = ring_z(half)
    w += [last, swap(last, "c")]

    p = soft(queries, resp_key, prefix)
    place = jnp.stack([x, yh, z, core]).astype(jnp.int32)
    acc, w_last = project(place, g[:7], w)
    gp, og, *s = front(lengths, acc, g[7], w_last, p, queries, resp_value, prefix)
    parts = lax.all_to_all(gp, ROLL, 0, 0, tiled=True)
    gq, grk, grv = back(og, s, p, queries, resp_key, prefix)
    total = jnp.sum(parts, axis=0)
    return gq, grk, grv, total[:, :HD], total[:, HD:]


def solution(mesh):
    torus = Mesh(mesh.devices.reshape(NZ, NY, 2, NX, 2), ROLL + TENSOR)
    placed = P(ROLL, TENSOR)
    return jax.shard_map(
        steps,
        mesh=torus,
        in_specs=(placed,) * 7 + (P(ROLL),),
        out_specs=(placed,) * 5,
        check_vma=False,
    )
```

```python
import jax
import jax.numpy as jnp
from jax import lax
from jax.experimental import pallas as pl
from jax.experimental.pallas import tpu as pltpu
from jax.sharding import Mesh
from jax.sharding import PartitionSpec as P

HD = 128
ROWS = 384
BLOCK = 128
GROUP = 4
PREFIX = 256
SCALE = HD**-0.5
KB = 640
TAIL = 16
F32 = jnp.float32
BF16 = jnp.bfloat16
ROLL = ("z", "yl", "c")
TENSOR = ("x", "yh")
NZ, NY, NX = 8, 4, 4
NT = (((1,), (1,)), ((), ()))


def swap(v, axis, bit=1):
    size = lax.axis_size(axis)
    return lax.ppermute(v, axis, [(i, i ^ bit) for i in range(size)])


def shift_x(v, step):
    return lax.ppermute(v, "x", [(x, (x + step) % NX) for x in range(NX)])


def ring_z(v):
    pairs = []
    for z in range(NZ):
        pairs.append((2 * z, 2 * ((z + 1) % NZ)))
        pairs.append((2 * z + 1, 2 * ((z - 1) % NZ) + 1))
    return lax.ppermute(v, ("z", "c"), pairs)


def in_pair(mine, other, bit, axis):
    first = jnp.where(bit == 0, mine, other)
    second = jnp.where(bit == 0, other, mine)
    return jnp.concatenate([first, second], axis=axis)


def stacked(ref, i):
    rows = slice(BLOCK * i, BLOCK * (i + 1))
    return jnp.concatenate([ref[rows, HD * h : HD * (h + 1)] for h in range(GROUP)], axis=0)


def prefix_part(ref, at):
    halves = [
        ref[TAIL * z : TAIL * (z + 1), 256 * half + at : 256 * half + at + HD]
        for z in range(NZ)
        for half in range(2)
    ]
    return jnp.concatenate(halves, axis=0)


def soft_rows(keys, q_ref, i):
    low = PREFIX + BLOCK * i
    scores = (
        lax.dot_general(keys[: low + BLOCK], stacked(q_ref, i), NT, preferred_element_type=F32)
        * SCALE
    )
    open_part = scores[:low]
    key_place = lax.broadcasted_iota(jnp.int32, (BLOCK, GROUP * BLOCK), 0)
    row_place = lax.broadcasted_iota(jnp.int32, (BLOCK, GROUP * BLOCK), 1) % BLOCK
    edge = jnp.where(key_place <= row_place, scores[low:], -jnp.inf)
    top = jnp.maximum(
        jnp.max(open_part, axis=0, keepdims=True), jnp.max(edge, axis=0, keepdims=True)
    )
    open_part = jnp.exp(open_part - top)
    edge = jnp.exp(edge - top)
    total = jnp.sum(open_part, axis=0, keepdims=True) + jnp.sum(edge, axis=0, keepdims=True)
    share = 1.0 / total
    return open_part * share, edge * share


def front_kernel(place_ref, length_ref, *refs):
    g_in, w_in, in_refs = refs[:8], refs[8:16], refs[16:19]
    gp_ref, out_refs = refs[19], refs[20:28]
    q_ref, rk_ref, rv_ref = refs[28:31]
    og_ref, s0, s1, s2, l0, l1, l2, pkv_ref = refs[31:39]
    g_buf, w_buf, p_buf0, p_buf1, p_buf2 = refs[39:44]
    sem, w_sem, tail_sem, out_sem, g_sem = refs[44:]
    small = [
        pltpu.make_async_copy(src, dst, sem.at[2 + k])
        for k, (src, dst) in enumerate(zip(in_refs, (q_ref, rk_ref, rv_ref)))
    ]
    outs = [
        pltpu.make_async_copy(src, dst, out_sem.at[k])
        for k, (src, dst) in enumerate(
            zip((og_ref, s0, s1, s2, l0, l1, l2, pkv_ref), out_refs)
        )
    ]
    yh, z, core, x = place_ref[0], place_ref[1], place_ref[2], place_ref[3]
    way = 1 - 2 * core
    p_bufs = (p_buf0, p_buf1, p_buf2)
    steps = (0, -way, -2 * way, -3 * way, 4, way, 2 * way, 3 * way)
    copies, tails = [], []
    for k, (src, step) in enumerate(zip(w_in, steps)):
        to = lax.rem(z + step + 8, 8)
        place = pl.ds(pl.multiple_of(TAIL * to, TAIL), TAIL)
        tails.append(
            pltpu.make_async_copy(src.at[pl.ds(KB, TAIL)], pkv_ref.at[place], tail_sem.at[k])
        )
        copies.append(pltpu.make_async_copy(src.at[pl.ds(0, KB)], w_buf.at[to], w_sem.at[k]))
    for k, src in enumerate(g_in):
        side = yh if k < 4 else 1 - yh
        dst = g_buf.at[side, lax.rem(x - (0, 1, 3, 2)[k % 4] + 4, 4)]
        copies.append(pltpu.make_async_copy(src, dst, g_sem.at[k]))
    for c in small + tails + copies:
        c.start()
    for c in small + tails:
        c.wait()
    outs[7].start()
    keys = jnp.concatenate([prefix_part(pkv_ref, 0), rk_ref[...]], axis=0)
    for i, (p_ref, l_ref) in enumerate(zip(p_bufs, (l0, l1, l2))):
        low = PREFIX + BLOCK * i
        open_part, edge = soft_rows(keys, q_ref, i)
        p_ref[:low], p_ref[low:] = open_part, edge
        if i:
            l_ref[: BLOCK * i] = open_part[PREFIX:].astype(BF16)
        l_ref[BLOCK * i :] = edge.astype(BF16)
        outs[4 + i].start()

    for c in copies:
        c.wait()
    grow = jnp.concatenate([g_buf[t % 2, t // 2] for t in range(8)], axis=1)
    total = jnp.dot(grow, w_buf[...].reshape(5120, 512), preferred_element_type=F32)
    row = lax.broadcasted_iota(jnp.int32, (ROWS, GROUP * HD), 0)
    out_grad = jnp.where(row < length_ref[0], total, 0.0).astype(BF16)
    for i in range(3):
        for h in range(GROUP):
            at = GROUP * BLOCK * i + BLOCK * h
            og_ref[at : at + BLOCK] = out_grad[
                BLOCK * i : BLOCK * (i + 1), HD * h : HD * (h + 1)
            ]
    outs[0].start()
    values = jnp.concatenate([prefix_part(pkv_ref, HD), rv_ref[...]], axis=0)
    key_grad = jnp.zeros((PREFIX, HD), F32)
    value_grad = jnp.zeros((PREFIX, HD), F32)
    for i, (p_ref, s_ref) in enumerate(zip(p_bufs, (s0, s1, s2))):
        width = PREFIX + BLOCK * (i + 1)
        grads = og_ref[GROUP * BLOCK * i : GROUP * BLOCK * (i + 1)]
        prob_grad = lax.dot_general(values[:width], grads, NT, preferred_element_type=F32)
        weights = p_ref[...]
        delta = jnp.sum(weights * prob_grad, axis=0, keepdims=True)
        score_low = (weights * (prob_grad - delta) * SCALE).astype(BF16)
        s_ref[...] = score_low
        outs[1 + i].start()
        key_grad += jnp.dot(score_low[:PREFIX], stacked(q_ref, i), preferred_element_type=F32)
        value_grad += jnp.dot(weights[:PREFIX].astype(BF16), grads, preferred_element_type=F32)
    for j in range(PREFIX // 4):
        gp_ref[j, :, :HD] = key_grad[4 * j : 4 * j + 4]
        gp_ref[j, :, HD:] = value_grad[4 * j : 4 * j + 4]
    for c in outs:
        c.wait()


def back_kernel(og_ref, s0, s1, s2, l0, l1, l2, q_ref, rk_ref, pkv_ref, gq_ref, grk_ref, grv_ref):
    keys = jnp.concatenate([prefix_part(pkv_ref, 0), rk_ref[...]], axis=0)
    keys_t = keys.astype(F32).T.astype(BF16)
    key_grad = [None] * 3
    value_grad = [None] * 3
    for i, (l_ref, s_ref) in enumerate(zip((l0, l1, l2), (s0, s1, s2))):
        width = PREFIX + BLOCK * (i + 1)
        rows = slice(BLOCK * i, BLOCK * (i + 1))
        score_low = s_ref[...]
        weights = l_ref[...]
        grads = og_ref[GROUP * BLOCK * i : GROUP * BLOCK * (i + 1)]
        kg = jnp.dot(score_low[PREFIX:], stacked(q_ref, i), preferred_element_type=F32)
        vg = jnp.dot(weights, grads, preferred_element_type=F32)
        qt = jnp.dot(keys_t[:, :width], score_low, preferred_element_type=F32)
        for h in range(GROUP):
            gq_ref[rows, HD * h : HD * (h + 1)] = qt[:, BLOCK * h : BLOCK * (h + 1)].T.astype(BF16)
        for j in range(i + 1):
            part = slice(BLOCK * j, BLOCK * (j + 1))
            key_grad[j] = kg[part] if key_grad[j] is None else key_grad[j] + kg[part]
            value_grad[j] = vg[part] if value_grad[j] is None else value_grad[j] + vg[part]
    for j in range(3):
        rows = slice(BLOCK * j, BLOCK * (j + 1))
        grk_ref[rows] = key_grad[j].astype(BF16)
        grv_ref[rows] = value_grad[j].astype(BF16)


VM = pl.BlockSpec(memory_space=pltpu.VMEM)
SM = pl.BlockSpec(memory_space=pltpu.SMEM)
ANY = pl.BlockSpec(memory_space=pl.ANY)
WIDTHS = tuple(PREFIX + BLOCK * (i + 1) for i in range(3))


def call(kernel, outs, in_specs, args, flops, scratch=(), out_specs=None):
    return pl.pallas_call(
        kernel,
        out_shape=[jax.ShapeDtypeStruct(s, d) for s, d in outs],
        in_specs=in_specs,
        out_specs=out_specs or [VM] * len(outs),
        scratch_shapes=scratch,
        cost_estimate=pl.CostEstimate(flops=flops, bytes_accessed=4000000, transcendentals=0),
    )(*args)


def front(place, lengths, g, w, queries, resp_key, resp_value):
    outs = [((64, 4, 2 * HD), F32), ((GROUP * ROWS, HD), BF16)]
    outs += [((w, GROUP * BLOCK), BF16) for w in WIDTHS]
    outs += [((w - PREFIX, GROUP * BLOCK), BF16) for w in WIDTHS]
    outs += [((NZ * TAIL, 512), BF16)]
    return call(
        front_kernel,
        outs,
        [SM] * 2 + [ANY] * 19,
        (place, lengths, *g, *w, queries, resp_key, resp_value),
        2 * 384 * 5120 * 512,
        [pltpu.VMEM((ROWS, n), BF16) for n in (512, HD, HD)]
        + [pltpu.VMEM(*o) for o in outs[1:]]
        + [pltpu.VMEM((2, NX, ROWS, KB), BF16), pltpu.VMEM((8, KB, 512), BF16)]
        + [pltpu.VMEM((w, GROUP * BLOCK), F32) for w in WIDTHS]
        + [pltpu.SemaphoreType.DMA((8,)) for _ in range(5)],
        [VM] + [ANY] * 8,
    )


def back(og, s, low, queries, resp_key, prefix):
    outs = [((ROWS, GROUP * HD), BF16), ((ROWS, HD), BF16), ((ROWS, HD), BF16)]
    return call(back_kernel, outs, [VM] * 10, (og, *s, *low, queries, resp_key, prefix), 1 << 30)


def steps(grad_out, out_weight, queries, resp_key, resp_value, prefix_key, prefix_value, lengths):
    x, yh, yl = lax.axis_index("x"), lax.axis_index("yh"), lax.axis_index("yl")
    z, core = lax.axis_index("z"), lax.axis_index("c")
    both = jnp.concatenate([prefix_key, prefix_value], axis=1)

    shard = jnp.concatenate([out_weight, jnp.pad(both, ((0, 4), (0, 256)))], axis=0)
    shards = [shard] + [swap(shard, "yl", k) for k in (1, 2, 3)]
    near = in_pair(shards[0], shards[1], yl % 2, 0)
    far = in_pair(shards[2], shards[3], yl % 2, 0)
    four = in_pair(near, far, yl // 2, 0).reshape(4, 1, 88, 512)
    pair = in_pair(four, swap(four, "c"), core, 1)
    tail = pair[:, :, 80:84, :256].reshape(2, TAIL, 256)
    piece = jnp.concatenate(
        [pair[:, :, :80].reshape(KB, 512), jnp.concatenate([tail[0], tail[1]], axis=1)], axis=0
    )
    def along_x(v):
        return [v] + [shift_x(v, k) for k in (1, 3, 2)]

    g = along_x(grad_out) + along_x(swap(grad_out, "yh"))
    aheads = [piece]
    for _ in range(4):
        aheads.append(ring_z(aheads[-1]))
    across = [swap(aheads[k], "c") for k in (1, 2, 3)]
    place = jnp.stack([yh, z, core, x]).astype(jnp.int32)
    gp, og, *rest = front(
        place, lengths, g, (*aheads, *across), queries, resp_key, resp_value
    )
    s, low, prefix = rest[:3], rest[3:6], rest[6]
    parts = lax.all_to_all(gp, ROLL, 0, 0, tiled=True)
    gq, grk, grv = back(og, s, low, queries, resp_key, prefix)
    total = jnp.sum(parts, axis=0)
    return gq, grk, grv, total[:, :HD], total[:, HD:]


def solution(mesh):
    torus = Mesh(mesh.devices.reshape(NZ, NY, 2, NX, 2), ROLL + TENSOR)
    placed = P(ROLL, TENSOR)
    return jax.shard_map(
        steps,
        mesh=torus,
        in_specs=(placed,) * 7 + (P(ROLL),),
        out_specs=(placed,) * 5,
        check_vma=False,
    )
```

```python
import jax
import jax.numpy as jnp
from jax import lax
from jax.experimental import pallas as pl
from jax.experimental.pallas import tpu as pltpu
from jax.sharding import Mesh
from jax.sharding import PartitionSpec as P

HD = 128
ROWS = 384
BLOCK = 128
GROUP = 4
PREFIX = 256
SCALE = HD**-0.5
KB = 640
TAIL = 16
PIECE = KB + TAIL
HALF = KB // 2
F32 = jnp.float32
BF16 = jnp.bfloat16
ROLL = ("z", "yl", "c")
TENSOR = ("x", "yh")
NZ, NY, NX = 8, 4, 4
NT = (((1,), (1,)), ((), ()))


def swap(v, axis, bit=1):
    size = lax.axis_size(axis)
    return lax.ppermute(v, axis, [(i, i ^ bit) for i in range(size)])


def shift_x(v, step):
    return lax.ppermute(v, "x", [(x, (x + step) % NX) for x in range(NX)])


def ring_z(v):
    pairs = []
    for z in range(NZ):
        pairs.append((2 * z, 2 * ((z + 1) % NZ)))
        pairs.append((2 * z + 1, 2 * ((z - 1) % NZ) + 1))
    return lax.ppermute(v, ("z", "c"), pairs)


def in_pair(mine, other, bit, axis):
    first = jnp.where(bit == 0, mine, other)
    second = jnp.where(bit == 0, other, mine)
    return jnp.concatenate([first, second], axis=axis)


def stacked(ref, i):
    rows = slice(BLOCK * i, BLOCK * (i + 1))
    return jnp.concatenate([ref[rows, HD * h : HD * (h + 1)] for h in range(GROUP)], axis=0)


def prefix_part(ref, at):
    halves = [
        ref[TAIL * z : TAIL * (z + 1), 256 * half + at : 256 * half + at + HD]
        for z in range(NZ)
        for half in range(2)
    ]
    return jnp.concatenate(halves, axis=0)


def soft_rows(keys, q_ref, i):
    low = PREFIX + BLOCK * i
    scores = (
        lax.dot_general(keys[: low + BLOCK], stacked(q_ref, i), NT, preferred_element_type=F32)
        * SCALE
    )
    open_part = scores[:low]
    key_place = lax.broadcasted_iota(jnp.int32, (BLOCK, GROUP * BLOCK), 0)
    row_place = lax.broadcasted_iota(jnp.int32, (BLOCK, GROUP * BLOCK), 1) % BLOCK
    edge = jnp.where(key_place <= row_place, scores[low:], -jnp.inf)
    top = jnp.maximum(
        jnp.max(open_part, axis=0, keepdims=True), jnp.max(edge, axis=0, keepdims=True)
    )
    open_part = jnp.exp(open_part - top)
    edge = jnp.exp(edge - top)
    total = jnp.sum(open_part, axis=0, keepdims=True) + jnp.sum(edge, axis=0, keepdims=True)
    share = 1.0 / total
    return open_part * share, edge * share


def front_kernel(length_ref, *refs):
    g_in, a_in, b_in, across = refs[:8], refs[8:13], refs[13:18], refs[18]
    q_ref, rk_ref, rv_ref = refs[19:22]
    gp_ref, out_refs = refs[22], refs[23:31]
    og_ref, s0, s1, s2, l0, l1, l2, pkv_ref = refs[31:39]
    w_buf, p_buf0, p_buf1, p_buf2, out_sem = refs[39:]
    outs = [
        pltpu.make_async_copy(src, dst, out_sem.at[k])
        for k, (src, dst) in enumerate(
            zip((og_ref, s0, s1, s2, l0, l1, l2, pkv_ref), out_refs)
        )
    ]
    yh, z = lax.axis_index("yh"), lax.axis_index("z")
    core, x = lax.axis_index("c"), lax.axis_index("x")
    way = 1 - 2 * core
    p_bufs = (p_buf0, p_buf1, p_buf2)
    steps = (0, -way, -2 * way, -3 * way, 4, way, 2 * way, 3 * way)
    for k, step in enumerate(steps):
        to = lax.rem(z + step + 8, 8)
        place = pl.ds(pl.multiple_of(TAIL * to, TAIL), TAIL)
        if k < 5:
            first, second, at, then = a_in[k], b_in[k], 0, 0
        else:
            first, second, at = across, across, (k - 5) * PIECE
            then = at + HALF + TAIL
        pkv_ref[place] = first[at + HALF : at + HALF + TAIL]
        w_buf[to, :HALF] = first[at : at + HALF]
        w_buf[to, HALF:] = second[then : then + HALF]
    outs[7].start()
    keys = jnp.concatenate([prefix_part(pkv_ref, 0), rk_ref[...]], axis=0)
    for i, (p_ref, l_ref) in enumerate(zip(p_bufs, (l0, l1, l2))):
        low = PREFIX + BLOCK * i
        open_part, edge = soft_rows(keys, q_ref, i)
        p_ref[:low], p_ref[low:] = open_part, edge
        if i:
            l_ref[: BLOCK * i] = open_part[PREFIX:].astype(BF16)
        l_ref[BLOCK * i :] = edge.astype(BF16)
        outs[4 + i].start()

    total = jnp.zeros((ROWS, 512), F32)
    for k, src in enumerate(g_in):
        side = yh if k < 4 else 1 - yh
        block = 2 * lax.rem(x - (0, 1, 3, 2)[k % 4] + 4, 4) + side
        total += jnp.dot(src[...], w_buf[block], preferred_element_type=F32)
    row = lax.broadcasted_iota(jnp.int32, (ROWS, GROUP * HD), 0)
    out_grad = jnp.where(row < length_ref[0], total, 0.0).astype(BF16)
    for i in range(3):
        for h in range(GROUP):
            at = GROUP * BLOCK * i + BLOCK * h
            og_ref[at : at + BLOCK] = out_grad[
                BLOCK * i : BLOCK * (i + 1), HD * h : HD * (h + 1)
            ]
    outs[0].start()
    values = jnp.concatenate([prefix_part(pkv_ref, HD), rv_ref[...]], axis=0)
    key_grad = jnp.zeros((PREFIX, HD), F32)
    value_grad = jnp.zeros((PREFIX, HD), F32)
    for i, (p_ref, s_ref) in enumerate(zip(p_bufs, (s0, s1, s2))):
        width = PREFIX + BLOCK * (i + 1)
        grads = og_ref[GROUP * BLOCK * i : GROUP * BLOCK * (i + 1)]
        prob_grad = lax.dot_general(values[:width], grads, NT, preferred_element_type=F32)
        weights = p_ref[...]
        delta = jnp.sum(weights * prob_grad, axis=0, keepdims=True)
        score_low = (weights * (prob_grad - delta) * SCALE).astype(BF16)
        s_ref[...] = score_low
        outs[1 + i].start()
        key_grad += jnp.dot(score_low[:PREFIX], stacked(q_ref, i), preferred_element_type=F32)
        value_grad += jnp.dot(weights[:PREFIX].astype(BF16), grads, preferred_element_type=F32)
    for j in range(PREFIX // 4):
        gp_ref[j, :, :HD] = key_grad[4 * j : 4 * j + 4].astype(BF16)
        gp_ref[j, :, HD:] = value_grad[4 * j : 4 * j + 4].astype(BF16)
    for c in outs:
        c.wait()


def back_kernel(og_ref, s0, s1, s2, l0, l1, l2, q_ref, rk_ref, pkv_ref, gq_ref, grk_ref, grv_ref):
    keys = jnp.concatenate([prefix_part(pkv_ref, 0), rk_ref[...]], axis=0)
    keys_t = keys.astype(F32).T.astype(BF16)
    key_grad = [None] * 3
    value_grad = [None] * 3
    for i, (l_ref, s_ref) in enumerate(zip((l0, l1, l2), (s0, s1, s2))):
        width = PREFIX + BLOCK * (i + 1)
        rows = slice(BLOCK * i, BLOCK * (i + 1))
        score_low = s_ref[...]
        weights = l_ref[...]
        grads = og_ref[GROUP * BLOCK * i : GROUP * BLOCK * (i + 1)]
        kg = jnp.dot(score_low[PREFIX:], stacked(q_ref, i), preferred_element_type=F32)
        vg = jnp.dot(weights, grads, preferred_element_type=F32)
        qt = jnp.dot(keys_t[:, :width], score_low, preferred_element_type=F32)
        for h in range(GROUP):
            gq_ref[rows, HD * h : HD * (h + 1)] = qt[:, BLOCK * h : BLOCK * (h + 1)].T.astype(BF16)
        for j in range(i + 1):
            part = slice(BLOCK * j, BLOCK * (j + 1))
            key_grad[j] = kg[part] if key_grad[j] is None else key_grad[j] + kg[part]
            value_grad[j] = vg[part] if value_grad[j] is None else value_grad[j] + vg[part]
    for j in range(3):
        rows = slice(BLOCK * j, BLOCK * (j + 1))
        grk_ref[rows] = key_grad[j].astype(BF16)
        grv_ref[rows] = value_grad[j].astype(BF16)


VM = pl.BlockSpec(memory_space=pltpu.VMEM)
SM = pl.BlockSpec(memory_space=pltpu.SMEM)
ANY = pl.BlockSpec(memory_space=pl.ANY)
VMEM_MIB = {"front": 34, "back": 59}
WIDTHS = tuple(PREFIX + BLOCK * (i + 1) for i in range(3))


def call(kernel, name, outs, in_specs, args, flops, scratch=(), out_specs=None):
    return pl.pallas_call(
        kernel,
        out_shape=[
            pltpu.HBM(s, d) if out_specs and k else jax.ShapeDtypeStruct(s, d)
            for k, (s, d) in enumerate(outs)
        ],
        in_specs=in_specs,
        out_specs=out_specs or [VM] * len(outs),
        scratch_shapes=scratch,
        cost_estimate=pl.CostEstimate(flops=flops, bytes_accessed=4000000, transcendentals=0),
        compiler_params=pltpu.CompilerParams(vmem_limit_bytes=VMEM_MIB[name] << 20),
    )(*args)


def front(lengths, g, w, queries, resp_key, resp_value):
    outs = [((64, 4, 2 * HD), BF16), ((GROUP * ROWS, HD), BF16)]
    outs += [((w, GROUP * BLOCK), BF16) for w in WIDTHS]
    outs += [((w - PREFIX, GROUP * BLOCK), BF16) for w in WIDTHS]
    outs += [((NZ * TAIL, 512), BF16)]
    return call(
        front_kernel,
        "front",
        outs,
        [SM] + [VM] * 22,
        (lengths, *g, *w, queries, resp_key, resp_value),
        2 * 384 * 5120 * 512,
        [pltpu.VMEM(*o) for o in outs[1:]]
        + [pltpu.VMEM((8, KB, 512), BF16)]
        + [pltpu.VMEM((w, GROUP * BLOCK), F32) for w in WIDTHS]
        + [pltpu.SemaphoreType.DMA((8,))],
        [VM] + [pl.BlockSpec(memory_space=pltpu.HBM)] * 8,
    )


def back(og, s, low, queries, resp_key, prefix):
    outs = [((ROWS, GROUP * HD), BF16), ((ROWS, HD), BF16), ((ROWS, HD), BF16)]
    return call(
        back_kernel, "back", outs, [VM] * 10, (og, *s, *low, queries, resp_key, prefix), 1 << 30
    )


def steps(grad_out, out_weight, queries, resp_key, resp_value, prefix_key, prefix_value, lengths):
    core = lax.axis_index("c")
    both = jnp.concatenate([prefix_key, prefix_value], axis=1)

    shard = jnp.concatenate([out_weight, jnp.pad(both, ((0, 4), (0, 256)))], axis=0)
    four = lax.all_to_all(jnp.broadcast_to(shard[None], (NY, 88, 512)), "yl", 0, 0, tiled=True)
    four = four[:, None]
    pair = in_pair(four, swap(four, "c"), core, 1)
    tail = pair[:, :, 80:84, :256].reshape(2, TAIL, 256)
    rows = pair[:, :, :80].reshape(KB, 512)
    tail = jnp.concatenate([tail[0], tail[1]], axis=1)
    near, then = [jnp.concatenate([rows[:HALF], tail], axis=0)], [rows[HALF:]]
    for _ in range(1, 5):
        near.append(ring_z(near[-1]))
        then.append(ring_z(then[-1]))

    def along_x(v):
        return [v] + [shift_x(v, k) for k in (1, 3, 2)]

    g = along_x(grad_out) + along_x(swap(grad_out, "yh"))
    joined = [half for k in (1, 2, 3) for half in (near[k], then[k])]
    joined = jnp.concatenate(joined, axis=0)
    across = swap(joined, "c")
    gp, og, *rest = front(
        lengths, g, (*near, *then, across), queries, resp_key, resp_value
    )
    s, low, prefix = rest[:3], rest[3:6], rest[6]
    parts = lax.all_to_all(gp, ROLL, 0, 0, tiled=True)
    gq, grk, grv = back(og, s, low, queries, resp_key, prefix)
    total = jnp.sum(parts.astype(F32), axis=0)
    return gq, grk, grv, total[:, :HD], total[:, HD:]


def solution(mesh):
    torus = Mesh(mesh.devices.reshape(NZ, NY, 2, NX, 2), ROLL + TENSOR)
    placed = P(ROLL, TENSOR)
    return jax.shard_map(
        steps,
        mesh=torus,
        in_specs=(placed,) * 7 + (P(ROLL),),
        out_specs=(placed,) * 5,
        check_vma=False,
    )
```

```python
import jax
import jax.numpy as jnp
from jax import lax
from jax.experimental import pallas as pl
from jax.experimental.pallas import tpu as pltpu
from jax.sharding import Mesh
from jax.sharding import PartitionSpec as P

HD = 128
ROWS = 384
BLOCK = 128
GROUP = 4
PREFIX = 256
SCALE = HD**-0.5
KB = 640
TAIL = 16
PIECE = KB + TAIL
HALF = KB // 2
F32 = jnp.float32
BF16 = jnp.bfloat16
ROLL = ("z", "yl", "c")
TENSOR = ("x", "yh")
NZ, NY, NX = 8, 4, 4
NT = (((1,), (1,)), ((), ()))


def swap(v, axis, bit=1):
    size = lax.axis_size(axis)
    return lax.ppermute(v, axis, [(i, i ^ bit) for i in range(size)])


def shift_x(v, step):
    return lax.ppermute(v, "x", [(x, (x + step) % NX) for x in range(NX)])


def ring_z(v):
    pairs = []
    for z in range(NZ):
        pairs.append((2 * z, 2 * ((z + 1) % NZ)))
        pairs.append((2 * z + 1, 2 * ((z - 1) % NZ) + 1))
    return lax.ppermute(v, ("z", "c"), pairs)


def in_pair(mine, other, bit, axis):
    first = jnp.where(bit == 0, mine, other)
    second = jnp.where(bit == 0, other, mine)
    return jnp.concatenate([first, second], axis=axis)


def stacked(ref, i):
    rows = slice(BLOCK * i, BLOCK * (i + 1))
    return jnp.concatenate([ref[rows, HD * h : HD * (h + 1)] for h in range(GROUP)], axis=0)


def prefix_part(ref, at):
    halves = [
        ref[TAIL * z : TAIL * (z + 1), 256 * half + at : 256 * half + at + HD]
        for z in range(NZ)
        for half in range(2)
    ]
    return jnp.concatenate(halves, axis=0)


def soft_rows(keys, q_ref, i):
    low = PREFIX + BLOCK * i
    scores = (
        lax.dot_general(keys[: low + BLOCK], stacked(q_ref, i), NT, preferred_element_type=F32)
        * SCALE
    )
    open_part = scores[:low]
    key_place = lax.broadcasted_iota(jnp.int32, (BLOCK, GROUP * BLOCK), 0)
    row_place = lax.broadcasted_iota(jnp.int32, (BLOCK, GROUP * BLOCK), 1) % BLOCK
    edge = jnp.where(key_place <= row_place, scores[low:], -jnp.inf)
    top = jnp.maximum(
        jnp.max(open_part, axis=0, keepdims=True), jnp.max(edge, axis=0, keepdims=True)
    )
    open_part = jnp.exp(open_part - top)
    edge = jnp.exp(edge - top)
    total = jnp.sum(open_part, axis=0, keepdims=True) + jnp.sum(edge, axis=0, keepdims=True)
    share = 1.0 / total
    return open_part * share, edge * share


def shard_kernel(w_ref, pk_ref, pv_ref, out_ref):
    for k in range(NY):
        out_ref[k, :80] = w_ref[...]
        out_ref[k, 80:88] = jnp.zeros((8, 512), BF16)
        out_ref[k, 80:84, :HD] = pk_ref[...]
        out_ref[k, 80:84, HD : 2 * HD] = pv_ref[...]


def front_kernel(length_ref, *refs):
    g_in, a_in, b_in, across = refs[:8], refs[8:13], refs[13:18], refs[18]
    q_ref, rk_ref, rv_ref = refs[19:22]
    gp_ref, out_refs = refs[22], refs[23:31]
    og_ref, s0, s1, s2, l0, l1, l2, pkv_ref = refs[31:39]
    w_buf, p_buf0, p_buf1, p_buf2, out_sem = refs[39:]
    outs = [
        pltpu.make_async_copy(src, dst, out_sem.at[k])
        for k, (src, dst) in enumerate(
            zip((og_ref, s0, s1, s2, l0, l1, l2, pkv_ref), out_refs)
        )
    ]
    yh, z = lax.axis_index("yh"), lax.axis_index("z")
    core, x = lax.axis_index("c"), lax.axis_index("x")
    way = 1 - 2 * core
    p_bufs = (p_buf0, p_buf1, p_buf2)
    steps = (0, -way, -2 * way, -3 * way, 4, way, 2 * way, 3 * way)
    for k, step in enumerate(steps):
        to = lax.rem(z + step + 8, 8)
        place = pl.ds(pl.multiple_of(TAIL * to, TAIL), TAIL)
        if k < 5:
            first, second, at, then = a_in[k], b_in[k], 0, 0
        else:
            first, second, at = across, across, (k - 5) * PIECE
            then = at + HALF + TAIL
        pkv_ref[place] = first[at + HALF : at + HALF + TAIL]
        w_buf[to, :HALF] = first[at : at + HALF]
        w_buf[to, HALF:] = second[then : then + HALF]
    outs[7].start()
    keys = jnp.concatenate([prefix_part(pkv_ref, 0), rk_ref[...]], axis=0)
    for i, (p_ref, l_ref) in enumerate(zip(p_bufs, (l0, l1, l2))):
        low = PREFIX + BLOCK * i
        open_part, edge = soft_rows(keys, q_ref, i)
        p_ref[:low], p_ref[low:] = open_part, edge
        if i:
            l_ref[: BLOCK * i] = open_part[PREFIX:].astype(BF16)
        l_ref[BLOCK * i :] = edge.astype(BF16)
        outs[4 + i].start()

    total = jnp.zeros((ROWS, 512), F32)
    for k, src in enumerate(g_in):
        side = yh if k < 4 else 1 - yh
        block = 2 * lax.rem(x - (0, 1, 3, 2)[k % 4] + 4, 4) + side
        total += jnp.dot(src[...], w_buf[block], preferred_element_type=F32)
    row = lax.broadcasted_iota(jnp.int32, (ROWS, GROUP * HD), 0)
    out_grad = jnp.where(row < length_ref[0], total, 0.0).astype(BF16)
    for i in range(3):
        for h in range(GROUP):
            at = GROUP * BLOCK * i + BLOCK * h
            og_ref[at : at + BLOCK] = out_grad[
                BLOCK * i : BLOCK * (i + 1), HD * h : HD * (h + 1)
            ]
    outs[0].start()
    values = jnp.concatenate([prefix_part(pkv_ref, HD), rv_ref[...]], axis=0)
    key_grad = jnp.zeros((PREFIX, HD), F32)
    value_grad = jnp.zeros((PREFIX, HD), F32)
    for i, (p_ref, s_ref) in enumerate(zip(p_bufs, (s0, s1, s2))):
        width = PREFIX + BLOCK * (i + 1)
        grads = og_ref[GROUP * BLOCK * i : GROUP * BLOCK * (i + 1)]
        prob_grad = lax.dot_general(values[:width], grads, NT, preferred_element_type=F32)
        weights = p_ref[...]
        delta = jnp.sum(weights * prob_grad, axis=0, keepdims=True)
        score_low = (weights * (prob_grad - delta) * SCALE).astype(BF16)
        s_ref[...] = score_low
        outs[1 + i].start()
        key_grad += jnp.dot(score_low[:PREFIX], stacked(q_ref, i), preferred_element_type=F32)
        value_grad += jnp.dot(weights[:PREFIX].astype(BF16), grads, preferred_element_type=F32)
    for j in range(PREFIX // 4):
        gp_ref[j, :, :HD] = key_grad[4 * j : 4 * j + 4].astype(BF16)
        gp_ref[j, :, HD:] = value_grad[4 * j : 4 * j + 4].astype(BF16)
    for c in outs:
        c.wait()


def back_kernel(og_ref, s0, s1, s2, l0, l1, l2, q_ref, rk_ref, pkv_ref, gq_ref, grk_ref, grv_ref):
    keys = jnp.concatenate([prefix_part(pkv_ref, 0), rk_ref[...]], axis=0)
    keys_t = keys.astype(F32).T.astype(BF16)
    key_grad = [None] * 3
    value_grad = [None] * 3
    for i, (l_ref, s_ref) in enumerate(zip((l0, l1, l2), (s0, s1, s2))):
        width = PREFIX + BLOCK * (i + 1)
        rows = slice(BLOCK * i, BLOCK * (i + 1))
        score_low = s_ref[...]
        weights = l_ref[...]
        grads = og_ref[GROUP * BLOCK * i : GROUP * BLOCK * (i + 1)]
        kg = jnp.dot(score_low[PREFIX:], stacked(q_ref, i), preferred_element_type=F32)
        vg = jnp.dot(weights, grads, preferred_element_type=F32)
        qt = jnp.dot(keys_t[:, :width], score_low, preferred_element_type=F32)
        for h in range(GROUP):
            gq_ref[rows, HD * h : HD * (h + 1)] = qt[:, BLOCK * h : BLOCK * (h + 1)].T.astype(BF16)
        for j in range(i + 1):
            part = slice(BLOCK * j, BLOCK * (j + 1))
            key_grad[j] = kg[part] if key_grad[j] is None else key_grad[j] + kg[part]
            value_grad[j] = vg[part] if value_grad[j] is None else value_grad[j] + vg[part]
    for j in range(3):
        rows = slice(BLOCK * j, BLOCK * (j + 1))
        grk_ref[rows] = key_grad[j].astype(BF16)
        grv_ref[rows] = value_grad[j].astype(BF16)


VM = pl.BlockSpec(memory_space=pltpu.VMEM)
SM = pl.BlockSpec(memory_space=pltpu.SMEM)
ANY = pl.BlockSpec(memory_space=pl.ANY)
VMEM_MIB = {"shard": 59, "front": 34, "back": 59}
WIDTHS = tuple(PREFIX + BLOCK * (i + 1) for i in range(3))


def call(kernel, name, outs, in_specs, args, flops, scratch=(), out_specs=None):
    return pl.pallas_call(
        kernel,
        out_shape=[
            pltpu.HBM(s, d) if out_specs and k else jax.ShapeDtypeStruct(s, d)
            for k, (s, d) in enumerate(outs)
        ],
        in_specs=in_specs,
        out_specs=out_specs or [VM] * len(outs),
        scratch_shapes=scratch,
        cost_estimate=pl.CostEstimate(flops=flops, bytes_accessed=4000000, transcendentals=0),
        compiler_params=pltpu.CompilerParams(vmem_limit_bytes=VMEM_MIB[name] << 20),
    )(*args)


def front(lengths, g, w, queries, resp_key, resp_value):
    outs = [((64, 4, 2 * HD), BF16), ((GROUP * ROWS, HD), BF16)]
    outs += [((w, GROUP * BLOCK), BF16) for w in WIDTHS]
    outs += [((w - PREFIX, GROUP * BLOCK), BF16) for w in WIDTHS]
    outs += [((NZ * TAIL, 512), BF16)]
    return call(
        front_kernel,
        "front",
        outs,
        [SM] + [VM] * 22,
        (lengths, *g, *w, queries, resp_key, resp_value),
        2 * 384 * 5120 * 512,
        [pltpu.VMEM(*o) for o in outs[1:]]
        + [pltpu.VMEM((8, KB, 512), BF16)]
        + [pltpu.VMEM((w, GROUP * BLOCK), F32) for w in WIDTHS]
        + [pltpu.SemaphoreType.DMA((8,))],
        [VM] + [pl.BlockSpec(memory_space=pltpu.HBM)] * 8,
    )


def shard(out_weight, prefix_key, prefix_value):
    outs = [((NY, 88, 512), BF16)]
    args = (out_weight, prefix_key, prefix_value)
    return call(shard_kernel, "shard", outs, [VM] * 3, args, 1 << 20)[0]


def back(og, s, low, queries, resp_key, prefix):
    outs = [((ROWS, GROUP * HD), BF16), ((ROWS, HD), BF16), ((ROWS, HD), BF16)]
    return call(
        back_kernel, "back", outs, [VM] * 10, (og, *s, *low, queries, resp_key, prefix), 1 << 30
    )


def steps(grad_out, out_weight, queries, resp_key, resp_value, prefix_key, prefix_value, lengths):
    core = lax.axis_index("c")
    copies = shard(out_weight, prefix_key, prefix_value)
    four = lax.all_to_all(copies, "yl", 0, 0, tiled=True)
    four = four[:, None]
    pair = in_pair(four, swap(four, "c"), core, 1)
    tail = pair[:, :, 80:84, :256].reshape(2, TAIL, 256)
    rows = pair[:, :, :80].reshape(KB, 512)
    tail = jnp.concatenate([tail[0], tail[1]], axis=1)
    near, then = [jnp.concatenate([rows[:HALF], tail], axis=0)], [rows[HALF:]]
    for _ in range(1, 5):
        near.append(ring_z(near[-1]))
        then.append(ring_z(then[-1]))

    def along_x(v):
        return [v] + [shift_x(v, k) for k in (1, 3, 2)]

    g = along_x(grad_out) + along_x(swap(grad_out, "yh"))
    joined = [half for k in (1, 2, 3) for half in (near[k], then[k])]
    joined = jnp.concatenate(joined, axis=0)
    across = swap(joined, "c")
    gp, og, *rest = front(
        lengths, g, (*near, *then, across), queries, resp_key, resp_value
    )
    s, low, prefix = rest[:3], rest[3:6], rest[6]
    parts = lax.all_to_all(gp, ROLL, 0, 0, tiled=True)
    gq, grk, grv = back(og, s, low, queries, resp_key, prefix)
    total = jnp.sum(parts.astype(F32), axis=0)
    return gq, grk, grv, total[:, :HD], total[:, HD:]


def solution(mesh):
    torus = Mesh(mesh.devices.reshape(NZ, NY, 2, NX, 2), ROLL + TENSOR)
    placed = P(ROLL, TENSOR)
    return jax.shard_map(
        steps,
        mesh=torus,
        in_specs=(placed,) * 7 + (P(ROLL),),
        out_specs=(placed,) * 5,
        check_vma=False,
    )
```
